32 devices in a mesh: pix: 8 (over z, x), frm: 4 (over y, core).
Axes of the slice: x: 2, y: 2, z: 4, core: 2. Of those that a mesh axis runs over, the one named last changes fastest.
Arguments:
- frames_y: bfloat16 [1024, 2048], P('pix', 'frm'), may hold values from -6 to 6
- traces: bfloat16 [1024, 2048], P('pix', 'frm'), may hold values from -0.13183594 to 0.13183594
- footprints: float32 [1024, 1024], P('pix'), may hold values from 0 to 2
- order: int32 [1024], replicated, may hold values from 0 to 1023, each once
- support: int32 [8, 256], P('pix'), may hold values from 0 to 1023, as said below
Outputs:
- footprints_new: float32 [1024, 1024], P('pix')
The draws below stay inside these ranges and needn't reach their ends.
Inputs may be any that keep to these rules, and one draw needn't show every extreme that they name: `support`: row j lists 256 different neurons; it governs pixels j * 128 to (j + 1) * 128 - 1.
All inputs are finite; a program needn't handle non-finite values.
Results may differ from the reference program's by a relative error of at most 0.0003.
Values may be sent and summed in bfloat16 or wider, within the bound.
No kernel may reach another device: no remote copies, remote signals or barrier semaphores. Data moves between devices by JAX's collectives and lax.ppermute only.
A program may use at most 64 MiB of HBM per device.

```python
import jax
import jax.numpy as jnp
from jax import lax

K = 1024
BLK = 128
SWEEPS = 3
SUPPORT = 256
PIX_DEV = 128
PIXELS = 1024
FRAMES = 2048
PIX_BLOCKS = 8


def draw_support(key, part):

    def one_row(row):
        listed = jax.random.permutation(jax.random.fold_in(jax.random.fold_in(key, 7301), row), K)
        return listed[:SUPPORT].astype(jnp.int32)
    return jax.vmap(one_row)(jnp.arange(PIX_BLOCKS, dtype=jnp.int32))


def levels(stream_key, extent, split, smallest, high):
    loudness = 1.0
    for dim, parts in split:
        heights = jax.random.uniform(jax.random.fold_in(jax.random.fold_in(stream_key, 6), dim), (parts,), jnp.float32, smallest / len(split), high / len(split))
        loudness = loudness * jnp.repeat(jnp.exp(heights), extent[dim] // parts).reshape((-1,) + (1,) * (len(extent) - 1 - dim))
    return loudness


def gaussian(own_key, shape, scale, bound, split=(), kind=jnp.bfloat16):
    array = scale * jax.random.normal(own_key, shape, jnp.float32)
    if split:
        array = array * levels(own_key, shape, split, -0.22, 0.18)
    return jnp.clip(array, -bound, bound).astype(kind)


def setup_inputs(seed: int = 0) -> dict:
    key_of = jax.random.split(jax.random.key(seed), 6)
    frames_y = gaussian(key_of[0], (PIXELS, FRAMES), 1.0, 6.0, ((0, 8), (1, 4)))
    traces = gaussian(key_of[1], (K, FRAMES), (FRAMES ** -0.5), 0.13183594, ((0, 8), (1, 4)))
    footprints = jnp.clip(2.0 * jax.random.uniform(key_of[2], (PIXELS, K), jnp.float32) ** levels(key_of[2], (PIXELS, K), ((0, 8),), -0.2, 0.2), 0.0, 2.0)
    order = jax.random.permutation(key_of[3], K).astype(jnp.int32)
    support = draw_support(jax.random.fold_in(key_of[5], 71), 0)
    return dict(frames_y=frames_y, traces=traces, footprints=footprints, order=order, support=support)


def reference(frames_y, traces, footprints, order, support):
    highest = lax.Precision.HIGHEST
    traces32 = traces.astype(jnp.float32)
    gram = jnp.dot(traces32, traces32.T, precision=highest)
    cross = jnp.dot(frames_y.astype(jnp.float32), traces32.T, precision=highest)
    neuron_ids = jnp.arange(K, dtype=jnp.int32)
    member = jnp.any(support[:, :, None] == neuron_ids[None, None, :], axis=1).astype(jnp.float32)
    keep = jnp.repeat(member, PIX_DEV, axis=0)
    current = jnp.take(footprints, order, axis=1)
    cross_perm = jnp.take(cross, order, axis=1)
    gram_perm = jnp.take(jnp.take(gram, order, axis=0), order, axis=1)
    keep_perm = jnp.take(keep, order, axis=1)
    diagonal = jnp.diagonal(gram_perm)
    for sweep_index in range(SWEEPS):
        for block_index in range(K // BLK):
            lower = block_index * BLK
            upper = lower + BLK
            numer = cross_perm[:, lower:upper] - jnp.dot(current, gram_perm[:, lower:upper], precision=highest)
            update = keep_perm[:, lower:upper] * jnp.maximum(current[:, lower:upper] + numer / diagonal[lower:upper], 0.0)
            scale = jnp.sqrt(lax.optimization_barrier(jnp.mean(update * update, axis=0)) + 1e-06)
            current = current.at[:, lower:upper].set(update / scale)
    return jnp.zeros_like(current).at[:, order].set(current)
```

```python
import functools

import jax
import jax.numpy as jnp
from jax import lax
from jax.experimental import pallas as pl
from jax.experimental.pallas import tpu as pltpu
from jax.sharding import PartitionSpec as P

BLK = 128
SWEEPS = 3
LANES = 128
VMEM_BYTES = 60 * 1024 * 1024


def spread(frames_y, traces, footprints, order, support):
    highest = lax.Precision.HIGHEST
    pix_rows = frames_y.shape[0]
    neurons = footprints.shape[1]
    total_pixels = pix_rows * lax.axis_size("pix")
    contract = (((1,), (1,)), ((), ()))
    stacked = jnp.concatenate([frames_y, traces], axis=0)
    terms = lax.dot_general(
        stacked,
        lax.all_gather(traces, "pix", axis=0, tiled=True),
        contract,
        preferred_element_type=jnp.float32,
    )
    cross, gram_part = lax.psum((terms[:pix_rows], terms[pix_rows:]), "frm")
    gram = lax.all_gather(gram_part, "pix", axis=0, tiled=True)
    neuron_ids = lax.iota(jnp.int32, neurons)
    member = jnp.any(support[0][:, None] == neuron_ids[None, :], axis=0).astype(jnp.float32)
    keep_perm = jnp.take(member, order)
    current = jnp.take(footprints, order, axis=1)
    cross_perm = jnp.take(cross, order, axis=1)
    gram_perm = jnp.take(jnp.take(gram, order, axis=0), order, axis=1)
    diagonal = jnp.diagonal(gram_perm)
    block_count = neurons // BLK
    for sweep_index in range(SWEEPS):
        for block_index in range(block_count):
            lower = block_index * BLK
            upper = lower + BLK
            numer = cross_perm[:, lower:upper] - jnp.dot(
                current, gram_perm[:, lower:upper], precision=highest
            )
            update = keep_perm[lower:upper] * jnp.maximum(
                current[:, lower:upper] + numer / diagonal[lower:upper], 0.0
            )
            squares = lax.psum(jnp.sum(update * update, axis=0), "pix")
            scale = jnp.sqrt(squares / total_pixels + 1e-06)
            current = current.at[:, lower:upper].set(update / scale)
    return jnp.zeros_like(current).at[:, order].set(current)


f32 = jnp.float32
bf16 = jnp.bfloat16


def dot(a, b):
    return jnp.dot(a, b, preferred_element_type=f32)


def dot_t(a, b):
    return lax.dot_general(a, b, (((1,), (1,)), ((), ())), preferred_element_type=f32)


def split2(x):
    hi = x.astype(bf16)
    return hi, (x - hi.astype(f32)).astype(bf16)


def split3(x):
    hi = x.astype(bf16)
    rest = x - hi.astype(f32)
    mid = rest.astype(bf16)
    return hi, mid, (rest - mid.astype(f32)).astype(bf16)


def join3(x):
    rows = x.shape[0] // 3
    return x[:rows] + x[rows : 2 * rows] + x[2 * rows :]


def as_column(row_ref):
    return jnp.broadcast_to(row_ref[...], (LANES, row_ref.shape[1])).T


def one_hot_into(out_ref, column, row_ref):
    for lower in range(0, row_ref.shape[1], LANES):
        hit = column == row_ref[:, lower : lower + LANES]
        out_ref[:, lower : lower + LANES] = jnp.where(hit, 1.0, 0.0).astype(bf16)


def gram_kernel(n, m, order_ref, ids_ref, support_ref, foot_ref, *refs):
    y_refs, refs = refs[:m], refs[m:]
    t_refs, refs = refs[: n * m], refs[n * m :]
    g_ref, own_ref, mine_ref = refs[:3]
    perm, members, t_all, y_all, t_perm, gram, split = refs[3:]
    neurons = order_ref.shape[1]
    rows, frames = t_refs[0].shape
    pixels = foot_ref.shape[0]
    me = lax.axis_index("frm")
    column = as_column(order_ref)
    one_hot_into(perm, column, ids_ref)
    one_hot_into(members, column, support_ref)
    for g in range(m):
        at = me ^ g
        y_all[at] = y_refs[g][...]
        for s in range(n):
            t_all[at, s * rows : (s + 1) * rows, :] = t_refs[s * m + g][...]
    for f in range(m):
        for lower in range(0, neurons, 256):
            part = dot(perm[lower : lower + 256, :], t_all[f])
            t_perm[lower : lower + 256, f * frames : (f + 1) * frames] = part.astype(bf16)
    for lower in range(0, neurons, 256):
        gram[lower : lower + 256, :] = dot_t(t_perm[lower : lower + 256, :], t_perm[...])
    cross = jnp.zeros((pixels, neurons), f32)
    for f in range(m):
        cross += dot_t(y_all[f], t_perm[:, f * frames : (f + 1) * frames])
    here = lax.axis_index("pix")
    foot = jnp.concatenate(
        [foot_ref[:, pl.ds(pl.multiple_of((here ^ s) * rows, rows), rows)] for s in range(n)],
        axis=1,
    )
    foot = join3(dot_t(jnp.concatenate(split3(foot), axis=0), perm[...]))
    foot_hl = jnp.concatenate(split2(foot), axis=0)
    eye = lax.broadcasted_iota(jnp.int32, (BLK, BLK), 0) == lax.broadcasted_iota(
        jnp.int32, (BLK, BLK), 1
    )
    for lower in range(0, neurons, BLK):
        upper = lower + BLK
        square = gram[lower:upper, lower:upper]
        inverse = 1.0 / jnp.sum(jnp.where(eye, square, 0.0), axis=0, keepdims=True)
        gram[lower:upper, lower:upper] = jnp.where(eye, 0.0, square)
        hi, lo = split2(gram[:, lower:upper] * inverse)
        g_ref[:, 2 * lower : 2 * lower + BLK] = hi
        g_ref[:, 2 * lower + BLK : 2 * upper] = lo
        right = cross[:, lower:upper] * inverse
        both = dot(foot_hl[:, lower:], g_ref[lower:, 2 * lower : 2 * upper])
        both = both[:pixels] + both[pixels:]
        first = right - (both[:, :BLK] + both[:, BLK:])
        for index, part in enumerate(split3(first)):
            split[index * 2 * pixels : index * 2 * pixels + pixels, lower:upper] = part
        for index, part in enumerate(split3(right)):
            split[index * 2 * pixels + pixels : (index + 1) * 2 * pixels, lower:upper] = part
    packed = join3(dot(split[...], members[...]))
    width = support_ref.shape[1]
    own_ref[:, :width] = packed[:pixels]
    own_ref[:, width:] = packed[pixels:]
    half = pixels // 2
    mine_ref[...] = own_ref[pl.ds((me % 2) * half, half), :]


def sweep_kernel(n, order_ref, ids_ref, own_ref, g_ref, *refs):
    s_refs, refs = refs[:n], refs[n:]
    mine_refs, refs = refs[: n - 1], refs[n - 1 :]
    other_refs, refs = refs[: n - 1], refs[n - 1 :]
    out_ref = refs[0]
    perm, members, packed, keep, first, right, cur_hi, cur_lo, fresh, result = refs[1:]
    neurons = order_ref.shape[1]
    pixels, width2 = own_ref.shape
    width = width2 // 2
    half = pixels // 2
    mine = lax.axis_index("frm") % 2
    column = as_column(order_ref)
    one_hot_into(perm, column, ids_ref)
    ones = jnp.ones((16, width), bf16)
    for s in range(n):
        one_hot_into(members, column, s_refs[s])
        if s == 0:
            packed[...] = own_ref[...]
        else:
            packed[pl.ds(mine * half, half), :] = mine_refs[s - 1][...]
            packed[pl.ds((1 - mine) * half, half), :] = other_refs[s - 1][...]
        stacked = jnp.concatenate(
            [part for x in (packed[:, :width], packed[:, width:]) for part in split3(x)] + [ones],
            axis=0,
        )
        wide = dot_t(stacked, members[...])
        rows = slice(s * pixels, (s + 1) * pixels)
        first[rows, :] = join3(wide[: 3 * pixels])
        right[rows, :] = join3(wide[3 * pixels : 6 * pixels])
        keep[s : s + 1, :] = wide[6 * pixels : 6 * pixels + 1]
    total = n * pixels

    def step(block, depth, source):
        lower, upper = block * BLK, (block + 1) * BLK
        squares = jnp.zeros((8, BLK), f32)
        for s in range(n):
            rows = slice(s * pixels, (s + 1) * pixels)
            value = source[rows, lower:upper]
            if depth:
                weights = g_ref[:depth, 2 * lower : 2 * upper]
                both = dot(cur_hi[rows, :depth], weights) + dot(cur_lo[rows, :depth], weights)
                value = value - (both[:, :BLK] + both[:, BLK:])
            value = keep[s : s + 1, lower:upper] * jnp.maximum(value, 0.0)
            fresh[rows, :] = value
            squares += jnp.sum((value * value).reshape(pixels // 8, 8, BLK), axis=0)
        mean = jnp.sum(squares, axis=0, keepdims=True) / total
        inverse = 1.0 / jnp.sqrt(mean + 1e-06)
        for s in range(n):
            rows = slice(s * pixels, (s + 1) * pixels)
            value = fresh[rows, :] * inverse
            if s == 0:
                result[:, lower:upper] = value
            hi, lo = split2(value)
            cur_hi[rows, lower:upper] = hi
            cur_lo[rows, lower:upper] = lo

    blocks = neurons // BLK
    for block in range(blocks):
        step(block, block * BLK, first)

    @pl.loop(0, SWEEPS - 1)
    def _(_):
        for block in range(blocks):
            step(block, neurons, right)

    out_ref[...] = join3(dot(jnp.concatenate(split3(result[...]), axis=0), perm[...]))


def replicated(n, m, frames_y, traces, footprints, order, support):
    pixels, frames = frames_y.shape
    rows = traces.shape[0]
    neurons = footprints.shape[1]
    width = support.shape[1]

    def swap(x, dp, df):
        pairs = [(p * m + f, (p ^ dp) * m + (f ^ df)) for p in range(n) for f in range(m)]
        return lax.ppermute(x, ("pix", "frm"), pairs)

    t, y = {(0, 0): traces}, {0: frames_y}
    for s in range(2, n, 2):
        t[s, 0] = swap(traces, s, 0)
    for g in range(2, m, 2):
        y[g] = swap(frames_y, 0, g)
    for s in range(0, n, 2):
        t[s + 1, 0] = swap(t[s, 0], 1, 0)
        for g in range(2, m, 2):
            t[s, g] = swap(t[s, 0], 0, g)
            if (s // 2) % 2 == 0:
                t[s + 1, g] = swap(t[s + 1, 0], 0, g)
            else:
                t[s + 1, g] = swap(t[s, g], 1, 0)
    for g in range(0, m, 2):
        y[g + 1] = swap(y[g], 0, 1)
        for s in range(n):
            t[s, g + 1] = swap(t[s, g], 0, 1)
    sup = [support] + [swap(support, s, 0) for s in range(1, n)]

    me = lax.axis_index("pix")
    order_row = order.reshape(1, neurons)
    lane = lax.iota(jnp.int32, neurons)
    ids = (((lane // rows) ^ me) * rows + lane % rows).reshape(1, neurons)
    vmem = pl.BlockSpec(memory_space=pltpu.VMEM)
    total = n * pixels
    params = pltpu.CompilerParams(vmem_limit_bytes=VMEM_BYTES)
    g, own, mine = pl.pallas_call(
        functools.partial(gram_kernel, n, m),
        out_shape=(
            jax.ShapeDtypeStruct((neurons, 2 * neurons), bf16),
            jax.ShapeDtypeStruct((pixels, 2 * width), f32),
            jax.ShapeDtypeStruct((pixels // 2, 2 * width), f32),
        ),
        in_specs=[vmem] * (4 + m + n * m),
        out_specs=(vmem, vmem, vmem),
        scratch_shapes=[
            pltpu.VMEM((neurons, neurons), bf16),
            pltpu.VMEM((neurons, width), bf16),
            pltpu.VMEM((m, neurons, frames), bf16),
            pltpu.VMEM((m, pixels, frames), bf16),
            pltpu.VMEM((neurons, m * frames), bf16),
            pltpu.VMEM((neurons, neurons), f32),
            pltpu.VMEM((6 * pixels, neurons), bf16),
        ],
        compiler_params=params,
        name="gram",
    )(
        order_row, ids, support, footprints,
        *[y[g] for g in range(m)],
        *[t[s, g] for s in range(n) for g in range(m)],
    )
    mines = [swap(mine, s, 0) for s in range(1, n)]
    others = [swap(x, 0, 1) for x in mines]
    natural = lane.reshape(1, neurons)
    return pl.pallas_call(
        functools.partial(sweep_kernel, n),
        out_shape=jax.ShapeDtypeStruct((pixels, neurons), f32),
        in_specs=[vmem] * (4 + n + 2 * (n - 1)),
        out_specs=vmem,
        scratch_shapes=[
            pltpu.VMEM((neurons, neurons), bf16),
            pltpu.VMEM((neurons, width), bf16),
            pltpu.VMEM((pixels, 2 * width), f32),
            pltpu.VMEM((n, neurons), f32),
            pltpu.VMEM((total, neurons), f32),
            pltpu.VMEM((total, neurons), f32),
            pltpu.VMEM((total, neurons), bf16),
            pltpu.VMEM((total, neurons), bf16),
            pltpu.VMEM((total, BLK), f32),
            pltpu.VMEM((pixels, neurons), f32),
        ],
        compiler_params=params,
        name="sweeps",
    )(order_row, natural, own, g, *sup, *mines, *others)


def power_of_two(x):
    return x > 1 and x & (x - 1) == 0


def solution(mesh):
    n, m = mesh.shape["pix"], mesh.shape["frm"]

    def local(frames_y, traces, footprints, order, support):
        neurons = footprints.shape[1]
        total = n * frames_y.shape[0]
        fits = 12 * total * neurons + 10 * neurons * neurons <= VMEM_BYTES // 2
        lined = neurons % 256 == 0 and traces.shape[0] % LANES == 0
        if fits and lined and power_of_two(n) and power_of_two(m):
            return replicated(n, m, frames_y, traces, footprints, order, support)
        return spread(frames_y, traces, footprints, order, support)

    in_specs = (P("pix", "frm"), P("pix", "frm"), P("pix", None), P(), P("pix", None))
    out_specs = P("pix", None)
    return jax.shard_map(local, mesh=mesh, in_specs=in_specs, out_specs=out_specs, check_vma=False)
```

```python
import functools

import jax
import jax.numpy as jnp
from jax import lax
from jax.experimental import pallas as pl
from jax.experimental.pallas import tpu as pltpu
from jax.sharding import PartitionSpec as P


BLK = 128
SWEEPS = 3
LANES = 128
EXTRA = 8
CHUNK = 512


VMEM_BYTES = 60 * 1024 * 1024


def spread(frames_y, traces, footprints, order, support):
    highest = lax.Precision.HIGHEST
    pix_rows = frames_y.shape[0]
    neurons = footprints.shape[1]
    total_pixels = pix_rows * lax.axis_size("pix")
    contract = (((1,), (1,)), ((), ()))
    stacked = jnp.concatenate([frames_y, traces], axis=0)
    terms = lax.dot_general(
        stacked,
        lax.all_gather(traces, "pix", axis=0, tiled=True),
        contract,
        preferred_element_type=jnp.float32,
    )
    cross, gram_part = lax.psum((terms[:pix_rows], terms[pix_rows:]), "frm")
    gram = lax.all_gather(gram_part, "pix", axis=0, tiled=True)
    neuron_ids = lax.iota(jnp.int32, neurons)
    member = jnp.any(support[0][:, None] == neuron_ids[None, :], axis=0).astype(jnp.float32)
    keep_perm = jnp.take(member, order)
    current = jnp.take(footprints, order, axis=1)
    cross_perm = jnp.take(cross, order, axis=1)
    gram_perm = jnp.take(jnp.take(gram, order, axis=0), order, axis=1)
    diagonal = jnp.diagonal(gram_perm)
    block_count = neurons // BLK
    for _ in range(SWEEPS):
        for block_index in range(block_count):
            lower = block_index * BLK
            upper = lower + BLK
            numer = cross_perm[:, lower:upper] - jnp.dot(
                current, gram_perm[:, lower:upper], precision=highest
            )
            update = keep_perm[lower:upper] * jnp.maximum(
                current[:, lower:upper] + numer / diagonal[lower:upper], 0.0
            )
            squares = lax.psum(jnp.sum(update * update, axis=0), "pix")
            scale = jnp.sqrt(squares / total_pixels + 1e-06)
            current = current.at[:, lower:upper].set(update / scale)
    return jnp.zeros_like(current).at[:, order].set(current)


f32 = jnp.float32
bf16 = jnp.bfloat16


def dot(a, b):
    return jnp.dot(a, b, preferred_element_type=f32)


def dot_t(a, b):
    return lax.dot_general(a, b, (((1,), (1,)), ((), ())), preferred_element_type=f32)


def split2(x):
    hi = x.astype(bf16)
    return hi, (x - hi.astype(f32)).astype(bf16)


def split3(x):
    hi = x.astype(bf16)
    rest = x - hi.astype(f32)
    mid = rest.astype(bf16)
    return hi, mid, (rest - mid.astype(f32)).astype(bf16)


def join3(x):
    rows = x.shape[0] // 3
    return x[:rows] + x[rows : 2 * rows] + x[2 * rows :]


def as_column(row_ref):
    return jnp.broadcast_to(row_ref[...], (LANES, row_ref.shape[1])).T


def one_hot_into(out_ref, column, row_ref):
    for lower in range(0, row_ref.shape[1], LANES):
        hit = column == row_ref[:, lower : lower + LANES]
        out_ref[:, lower : lower + LANES] = jnp.where(hit, 1.0, 0.0).astype(bf16)


def setup_kernel(order_ref, ids_ref, support_ref, foot_ref, frames_ref, traces_ref, *outs):
    column_ref, perm, members, foot_hl, listed, frames_out, traces_out = outs
    frames_out[...] = frames_ref[...]
    traces_out[...] = traces_ref[...]
    pixels = foot_ref.shape[0]
    width = support_ref.shape[1]
    column = as_column(order_ref)
    column_ref[...] = column
    one_hot_into(perm, column, ids_ref)
    one_hot_into(members, column, support_ref)
    foot = join3(dot_t(jnp.concatenate(split3(foot_ref[...]), axis=0), perm[...]))
    hi, lo = split2(foot)
    foot_hl[:pixels, :] = hi
    foot_hl[pixels:, :] = lo
    ids = jnp.broadcast_to(support_ref[...].astype(f32), (EXTRA, width))
    listed[...] = jnp.concatenate([ids, ids], axis=1)


def gram_kernel(m, held, rows, perm, members, foot_hl, listed, *refs):
    y_refs, refs = refs[:m], refs[m:]
    t_refs, refs = refs[: len(held)], refs[len(held) :]
    g_ref, own_ref, mine_ref = refs[:3]
    t_all, y_all, t_perm, gram, split = refs[3:]
    neurons = perm.shape[0]
    pixels, frames = y_refs[0].shape
    me, here = lax.axis_index("frm"), lax.axis_index("pix")
    for g in range(m):
        y_all[me ^ g] = y_refs[g][...]
    for names, ref in zip(held, t_refs):
        for place, (s, g) in enumerate(names):
            to = pl.ds(pl.multiple_of((here ^ s) * rows, rows), rows)
            t_all[me ^ g, to, :] = ref[place * rows : (place + 1) * rows, :]
    for f in range(m):
        for lower in range(0, neurons, 256):
            part = dot(perm[lower : lower + 256, :], t_all[f])
            t_perm[lower : lower + 256, f * frames : (f + 1) * frames] = part.astype(bf16)
    for lower in range(0, neurons, 256):
        gram[lower : lower + 256, :] = dot_t(t_perm[lower : lower + 256, :], t_perm[...])
    cross = jnp.zeros((pixels, neurons), f32)
    for f in range(m):
        cross += dot_t(y_all[f], t_perm[:, f * frames : (f + 1) * frames])
    eye = lax.broadcasted_iota(jnp.int32, (BLK, BLK), 0) == lax.broadcasted_iota(
        jnp.int32, (BLK, BLK), 1
    )
    for lower in range(0, neurons, BLK):
        upper = lower + BLK
        square = gram[lower:upper, lower:upper]
        inverse = 1.0 / jnp.sum(jnp.where(eye, square, 0.0), axis=0, keepdims=True)
        gram[lower:upper, lower:upper] = jnp.where(eye, 0.0, square)
        hi, lo = split2(gram[:, lower:upper] * inverse)
        g_ref[:, 2 * lower : 2 * lower + BLK] = hi
        g_ref[:, 2 * lower + BLK : 2 * upper] = lo
        right = cross[:, lower:upper] * inverse
        both = dot(foot_hl[:, lower:], g_ref[lower:, 2 * lower : 2 * upper])
        both = both[:pixels] + both[pixels:]
        first = right - (both[:, :BLK] + both[:, BLK:])
        for index, part in enumerate(split3(first)):
            split[index * 2 * pixels : index * 2 * pixels + pixels, lower:upper] = part
        for index, part in enumerate(split3(right)):
            split[index * 2 * pixels + pixels : (index + 1) * 2 * pixels, lower:upper] = part
    packed = join3(dot(split[...], members[...]))
    width = members.shape[1]
    own_ref[:, :width] = packed[:pixels]
    own_ref[:, width:] = packed[pixels:]
    half = pixels // 2
    mine_ref[:half, :] = own_ref[pl.ds((me % 2) * half, half), :]
    mine_ref[half:, :] = listed[...]


def sweep_kernel(n, column_ref, perm, mine_members, own_ref, g_ref, *refs):
    mine_refs, refs = refs[: n - 1], refs[n - 1 :]
    other_refs, refs = refs[: n - 1], refs[n - 1 :]
    out_ref = refs[0]
    members, packed, keep, first, right, weights, cur, ahead, fresh, result = refs[1:]
    neurons = perm.shape[0]
    pixels, width2 = own_ref.shape
    width = width2 // 2
    half = pixels // 2
    blocks = neurons // BLK
    mine = lax.axis_index("frm") % 2
    column = column_ref[...]
    for block in range(blocks):
        piece = g_ref[block * BLK : (block + 1) * BLK, :]
        weights[2 * block * BLK : (2 * block + 1) * BLK, :] = piece
        weights[(2 * block + 1) * BLK : 2 * (block + 1) * BLK, :] = piece
    ones = jnp.ones((16, width), bf16)
    for s in range(n):
        if s == 0:
            packed[...] = own_ref[...]
            members[...] = mine_members[...]
        else:
            packed[pl.ds(mine * half, half), :] = mine_refs[s - 1][:half, :]
            packed[pl.ds((1 - mine) * half, half), :] = other_refs[s - 1][:half, :]
            listed = mine_refs[s - 1][half : half + 1, :width].astype(jnp.int32)
            one_hot_into(members, column, listed)
        stacked = jnp.concatenate(
            [part for x in (packed[:, :width], packed[:, width:]) for part in split3(x)] + [ones],
            axis=0,
        )
        wide = dot_t(stacked, members[...])
        rows = slice(s * pixels, (s + 1) * pixels)
        first[rows, :] = join3(wide[: 3 * pixels])
        right[rows, :] = join3(wide[3 * pixels : 6 * pixels])
        keep[s : s + 1, :] = wide[6 * pixels : 6 * pixels + 1]
    total = n * pixels

    def tile(block):
        return slice(2 * block * BLK, 2 * (block + 1) * BLK)

    def look_ahead(block, spans, slot):
        for start in range(0, total, CHUNK):
            rows = slice(start, start + CHUNK)
            terms = [
                dot(cur[rows, 2 * lower * BLK : 2 * upper * BLK],
                    weights[2 * lower * BLK : 2 * upper * BLK, tile(block)])
                for lower, upper in spans if upper > lower
            ]
            if terms:
                both = sum(terms[1:], terms[0])
                ahead[slot, rows, :] = both[:, :BLK] + both[:, BLK:]

    def step(block, previous, has_ahead, source, next_block, next_spans):
        lower, upper = block * BLK, (block + 1) * BLK
        squares = jnp.zeros((8, BLK), f32)
        if previous is not None:
            for start in range(0, total, CHUNK):
                rows = slice(start, start + CHUNK)
                both = dot(cur[rows, tile(previous)], weights[tile(previous), tile(block)])
                fresh[rows, :] = both[:, :BLK] + both[:, BLK:]
        for s in range(n):
            rows = slice(s * pixels, (s + 1) * pixels)
            value = source[rows, lower:upper]
            if has_ahead:
                value = value - ahead[block % 2, rows, :]
            if previous is not None:
                value = value - fresh[rows, :]
            value = keep[s : s + 1, lower:upper] * jnp.maximum(value, 0.0)
            fresh[rows, :] = value
            squares += jnp.sum((value * value).reshape(pixels // 8, 8, BLK), axis=0)
        if next_block is not None:
            look_ahead(next_block, next_spans, next_block % 2)
        mean = jnp.sum(squares, axis=0, keepdims=True) / total
        inverse = 1.0 / jnp.sqrt(mean + 1e-06)
        for s in range(n):
            rows = slice(s * pixels, (s + 1) * pixels)
            value = fresh[rows, :] * inverse
            if s == 0:
                result[:, lower:upper] = value
            hi, lo = split2(value)
            cur[rows, 2 * lower : 2 * lower + BLK] = hi
            cur[rows, 2 * lower + BLK : 2 * upper] = lo

    last = blocks - 1
    for block in range(blocks):
        previous = block - 1 if block else None
        if block < last:
            step(block, previous, block > 1, first, block + 1, [(0, block)])
        else:
            step(block, previous, block > 1, first, 0, [(0, last)])

    @pl.loop(0, SWEEPS - 1)
    def _(_):
        for block in range(blocks):
            after = (block + 1) % blocks
            spans = [(0, block), (block + 1, blocks)]
            step(block, (block - 1) % blocks, True, right, after, spans)

    out_ref[...] = join3(dot(jnp.concatenate(split3(result[...]), axis=0), perm[...]))


def replicated(n, m, frames_y, traces, footprints, order, support):
    pixels, frames = frames_y.shape
    rows = traces.shape[0]
    neurons = footprints.shape[1]
    width = support.shape[1]

    def swap(x, dp, df):
        pairs = [(p * m + f, (p ^ dp) * m + (f ^ df)) for p in range(n) for f in range(m)]
        return lax.ppermute(x, ("pix", "frm"), pairs)

    def stack(xs):
        return jnp.concatenate(xs, axis=0) if len(xs) > 1 else xs[0]

    shape = jax.ShapeDtypeStruct
    vmem = pl.BlockSpec(memory_space=pltpu.VMEM)
    total = n * pixels

    def call(kernel, flops, outs, scratch, limit, *args):
        moving = sum(x.size * x.dtype.itemsize for x in args)
        return pl.pallas_call(
            kernel,
            out_shape=outs,
            in_specs=[vmem] * len(args),
            out_specs=jax.tree.map(lambda _: vmem, outs),
            scratch_shapes=[pltpu.VMEM(*x) for x in scratch],
            compiler_params=pltpu.CompilerParams(vmem_limit_bytes=limit * VMEM_BYTES // 60),
            cost_estimate=pl.CostEstimate(flops=flops, bytes_accessed=moving, transcendentals=0),
        )(*args)

    order_row = order.reshape(1, neurons)
    natural = lax.iota(jnp.int32, neurons).reshape(1, neurons)
    bits = [1 << k for k in range(n.bit_length() - 2, 0, -1)]
    far = {0: traces}
    for bit in bits:
        far[bit] = swap(traces, bit, 0)
    blobs, y = [], {0: frames_y}

    def beside(names, blob):
        blobs.append(([(s, g ^ 1) for s, g in names], swap(blob, 0, 1)))

    def named(group, ds, dg):
        return [(s ^ ds, dg) for s in group]

    def spread_near(group, blob, way):
        along = swap(blob, 1, 0)
        near, relays = [(named(group, 1, 0), along)], []
        for g in range(2, m, 2):
            across = swap(blob, 0, g)
            near.append((named(group, 0, g), across))
            if way == "direct":
                near.append((named(group, 1, g), swap(blob, 1, g)))
            else:
                hop = (across, 1, 0) if way == "x" else (along, 0, g)
                relays.append((named(group, 1, g), hop))
        return near, relays

    own_near, own_relays = spread_near([0], traces, "y")
    for g in range(2, m, 2):
        y[g] = swap(frames_y, 0, g)
    singles = []
    for bit in bits[1:]:
        for s in [s for s in far if s & -s > bit]:
            far[s ^ bit] = swap(far[s], bit, 0)
            singles.append(s ^ bit)
    pair, relays = [], []
    if bits:
        pair_blob = stack([far[bit] for bit in bits])
        pair, relays = spread_near(bits, pair_blob, "x")
    own_near += [(names, swap(*hop)) for names, hop in own_relays]
    beside([(0, 0)], traces)
    for g in range(0, m, 2):
        y[g + 1] = swap(y[g], 0, 1)
    if bits:
        beside(named(bits, 0, 0), pair_blob)
        blobs.append((named(bits, 0, 0), pair_blob))
    later = []
    for s in singles:
        near, _ = spread_near([s], far[s], "direct")
        later += near
        beside([(s, 0)], far[s])
        blobs.append(([(s, 0)], far[s]))
    pair += [(names, swap(*hop)) for names, hop in relays]
    column, perm, members, foot_hl, listed, own_frames, traces_here = call(
        setup_kernel,
        6 * pixels * neurons * neurons,
        (
            shape((neurons, LANES), jnp.int32),
            shape((neurons, neurons), bf16),
            shape((neurons, width), bf16),
            shape((2 * pixels, neurons), bf16),
            shape((EXTRA, 2 * width), f32),
            shape((pixels, frames), bf16),
            shape((rows, frames), bf16),
        ),
        [],
        16,
        order_row, natural, support, footprints, frames_y, traces,
    )
    for entry in own_near + pair + later:
        beside(*entry)
    blobs += [([(0, 0)], traces_here)] + own_near + pair + later

    g, own, mine = call(
        functools.partial(gram_kernel, m, [names for names, _ in blobs], rows),
        4 * neurons * neurons * m * frames,
        (
            shape((neurons, 2 * neurons), bf16),
            shape((pixels, 2 * width), f32),
            shape((pixels // 2 + EXTRA, 2 * width), f32),
        ),
        [
            ((m, neurons, frames), bf16),
            ((m, pixels, frames), bf16),
            ((neurons, m * frames), bf16),
            ((neurons, neurons), f32),
            ((6 * pixels, neurons), bf16),
        ],
        36,
        perm, members, foot_hl, listed,
        own_frames,
        *[y[k] for k in range(1, m)],
        *[blob for _, blob in blobs],
    )
    got = {0: mine}
    for bit in bits:
        got[bit] = swap(mine, bit, 0)
    got[1] = swap(mine, 1, 0)
    others = {}
    for bit in bits[::-1]:
        got[bit ^ 1] = swap(got[bit], 1, 0)
        if bit != bits[0]:
            for s in [s for s in list(got) if s & -s > bit]:
                got[s ^ bit] = swap(got[s], bit, 0)
    for s in list(got):
        if s and s ^ 1 not in got:
            got[s ^ 1] = swap(got[s], 1, 0)
    for s in got:
        if s:
            others[s] = swap(got[s], 0, 1)
    mines = [got[s] for s in range(1, n)]
    others = [others[s] for s in range(1, n)]
    return call(
        functools.partial(sweep_kernel, n),
        2 * SWEEPS * 4 * total * neurons * neurons,
        shape((pixels, neurons), f32),
        [
            ((neurons, width), bf16),
            ((pixels, 2 * width), f32),
            ((n, neurons), f32),
            ((total, neurons), f32),
            ((total, neurons), f32),
            ((2 * neurons, 2 * neurons), bf16),
            ((total, 2 * neurons), bf16),
            ((2, total, BLK), f32),
            ((total, BLK), f32),
            ((pixels, neurons), f32),
        ],
        40,
        column, perm, members, own, g, *mines, *others,
    )


def power_of_two(x):
    return x > 1 and x & (x - 1) == 0


def solution(mesh):
    n, m = mesh.shape["pix"], mesh.shape["frm"]

    def local(frames_y, traces, footprints, order, support):
        neurons = footprints.shape[1]
        total = n * frames_y.shape[0]
        fits = 12 * total * neurons + 10 * neurons * neurons <= VMEM_BYTES // 2
        lined = neurons % 256 == 0 and traces.shape[0] % LANES == 0
        if fits and lined and power_of_two(n) and power_of_two(m):
            return replicated(n, m, frames_y, traces, footprints, order, support)
        return spread(frames_y, traces, footprints, order, support)

    in_specs = (P("pix", "frm"), P("pix", "frm"), P("pix", None), P(), P("pix", None))
    out_specs = P("pix", None)
    return jax.shard_map(local, mesh=mesh, in_specs=in_specs, out_specs=out_specs, check_vma=False)
```

```python
import functools

import jax
import jax.numpy as jnp
from jax import lax
from jax.experimental import pallas as pl
from jax.experimental.pallas import tpu as pltpu
from jax.sharding import PartitionSpec as P


BLK = 128
SWEEPS = 3
LANES = 128
EXTRA = 8
CHUNK = 512
UNPACK_MIB = 16
SWEEP_MIB = 16


VMEM_BYTES = 60 * 1024 * 1024


def spread(frames_y, traces, footprints, order, support):
    highest = lax.Precision.HIGHEST
    pix_rows = frames_y.shape[0]
    neurons = footprints.shape[1]
    total_pixels = pix_rows * lax.axis_size("pix")
    contract = (((1,), (1,)), ((), ()))
    stacked = jnp.concatenate([frames_y, traces], axis=0)
    terms = lax.dot_general(
        stacked,
        lax.all_gather(traces, "pix", axis=0, tiled=True),
        contract,
        preferred_element_type=jnp.float32,
    )
    cross, gram_part = lax.psum((terms[:pix_rows], terms[pix_rows:]), "frm")
    gram = lax.all_gather(gram_part, "pix", axis=0, tiled=True)
    neuron_ids = lax.iota(jnp.int32, neurons)
    member = jnp.any(support[0][:, None] == neuron_ids[None, :], axis=0).astype(jnp.float32)
    keep_perm = jnp.take(member, order)
    current = jnp.take(footprints, order, axis=1)
    cross_perm = jnp.take(cross, order, axis=1)
    gram_perm = jnp.take(jnp.take(gram, order, axis=0), order, axis=1)
    diagonal = jnp.diagonal(gram_perm)
    block_count = neurons // BLK
    for _ in range(SWEEPS):
        for block_index in range(block_count):
            lower = block_index * BLK
            upper = lower + BLK
            numer = cross_perm[:, lower:upper] - jnp.dot(
                current, gram_perm[:, lower:upper], precision=highest
            )
            update = keep_perm[lower:upper] * jnp.maximum(
                current[:, lower:upper] + numer / diagonal[lower:upper], 0.0
            )
            squares = lax.psum(jnp.sum(update * update, axis=0), "pix")
            scale = jnp.sqrt(squares / total_pixels + 1e-06)
            current = current.at[:, lower:upper].set(update / scale)
    return jnp.zeros_like(current).at[:, order].set(current)


f32 = jnp.float32
bf16 = jnp.bfloat16


def dot(a, b):
    return jnp.dot(a, b, preferred_element_type=f32)


def dot_t(a, b):
    return lax.dot_general(a, b, (((1,), (1,)), ((), ())), preferred_element_type=f32)


def split2(x):
    hi = x.astype(bf16)
    return hi, (x - hi.astype(f32)).astype(bf16)


def split3(x):
    hi = x.astype(bf16)
    rest = x - hi.astype(f32)
    mid = rest.astype(bf16)
    return hi, mid, (rest - mid.astype(f32)).astype(bf16)


def join3(x):
    rows = x.shape[0] // 3
    return x[:rows] + x[rows : 2 * rows] + x[2 * rows :]


def as_column(row_ref):
    return jnp.broadcast_to(row_ref[...], (LANES, row_ref.shape[1])).T


def one_hot_into(out_ref, column, row_ref):
    for lower in range(0, row_ref.shape[1], LANES):
        hit = column == row_ref[:, lower : lower + LANES]
        out_ref[:, lower : lower + LANES] = jnp.where(hit, 1.0, 0.0).astype(bf16)


def setup_kernel(order_ref, ids_ref, support_ref, foot_ref, frames_ref, traces_ref, *outs):
    column_ref, perm, members, foot_hl, listed, frames_out, traces_out = outs
    frames_out[...] = frames_ref[...]
    traces_out[...] = traces_ref[...]
    pixels = foot_ref.shape[0]
    width = support_ref.shape[1]
    column = as_column(order_ref)
    column_ref[...] = column
    one_hot_into(perm, column, ids_ref)
    one_hot_into(members, column, support_ref)
    foot = join3(dot_t(jnp.concatenate(split3(foot_ref[...]), axis=0), perm[...]))
    hi, lo = split2(foot)
    foot_hl[:pixels, :] = hi
    foot_hl[pixels:, :] = lo
    ids = jnp.broadcast_to(support_ref[...].astype(f32), (EXTRA, width))
    listed[...] = jnp.concatenate([ids, ids], axis=1)


def gram_kernel(m, held, rows, perm, members, foot_hl, listed, *refs):
    y_refs, refs = refs[:m], refs[m:]
    t_refs, refs = refs[: len(held)], refs[len(held) :]
    g_ref, own_ref, mine_ref = refs[:3]
    t_all, y_all, t_perm, gram, split = refs[3:]
    neurons = perm.shape[0]
    pixels, frames = y_refs[0].shape
    me, here = lax.axis_index("frm"), lax.axis_index("pix")
    for g in range(m):
        y_all[me ^ g] = y_refs[g][...]
    for names, ref in zip(held, t_refs):
        for place, (s, g) in enumerate(names):
            to = pl.ds(pl.multiple_of((here ^ s) * rows, rows), rows)
            t_all[me ^ g, to, :] = ref[place * rows : (place + 1) * rows, :]
    for f in range(m):
        for lower in range(0, neurons, 256):
            part = dot(perm[lower : lower + 256, :], t_all[f])
            t_perm[lower : lower + 256, f * frames : (f + 1) * frames] = part.astype(bf16)
    for lower in range(0, neurons, 256):
        gram[lower : lower + 256, :] = dot_t(t_perm[lower : lower + 256, :], t_perm[...])
    cross = jnp.zeros((pixels, neurons), f32)
    for f in range(m):
        cross += dot_t(y_all[f], t_perm[:, f * frames : (f + 1) * frames])
    eye = lax.broadcasted_iota(jnp.int32, (BLK, BLK), 0) == lax.broadcasted_iota(
        jnp.int32, (BLK, BLK), 1
    )
    for lower in range(0, neurons, BLK):
        upper = lower + BLK
        square = gram[lower:upper, lower:upper]
        inverse = 1.0 / jnp.sum(jnp.where(eye, square, 0.0), axis=0, keepdims=True)
        gram[lower:upper, lower:upper] = jnp.where(eye, 0.0, square)
        hi, lo = split2(gram[:, lower:upper] * inverse)
        g_ref[:, 2 * lower : 2 * lower + BLK] = hi
        g_ref[:, 2 * lower + BLK : 2 * upper] = lo
        right = cross[:, lower:upper] * inverse
        both = dot(foot_hl[:, lower:], g_ref[lower:, 2 * lower : 2 * upper])
        both = both[:pixels] + both[pixels:]
        first = right - (both[:, :BLK] + both[:, BLK:])
        for index, part in enumerate(split3(first)):
            split[index * 2 * pixels : index * 2 * pixels + pixels, lower:upper] = part
        for index, part in enumerate(split3(right)):
            split[index * 2 * pixels + pixels : (index + 1) * 2 * pixels, lower:upper] = part
    packed = join3(dot(split[...], members[...]))
    width = members.shape[1]
    own_ref[:, :width] = packed[:pixels]
    own_ref[:, width:] = packed[pixels:]
    half = pixels // 2
    mine_ref[:half, :] = own_ref[pl.ds((me % 2) * half, half), :]
    mine_ref[half:, :] = listed[...]


def unpack_kernel(blocks_at, mine_at, *refs):
    column_ref, refs = refs[0], refs[1:]
    inputs, outs = refs[: mine_at], refs[mine_at:]
    first, right, keep = outs[:3]
    members, packed = outs[-2:]
    column = column_ref[...]
    pixels, width2 = packed.shape
    width, half = width2 // 2, pixels // 2
    mine = lax.axis_index("frm") % 2
    ones = jnp.ones((16, width), bf16)
    at = 0
    for place, own in enumerate(blocks_at):
        if own:
            packed[...] = inputs[at][...]
            members[...] = inputs[at + 1][...]
            g_ref, weights = inputs[at + 2], outs[3]
            for lower in range(0, g_ref.shape[0], BLK):
                piece = g_ref[lower : lower + BLK, :]
                weights[2 * lower : 2 * lower + BLK, :] = piece
                weights[2 * lower + BLK : 2 * (lower + BLK), :] = piece
            at += 3
        else:
            packed[pl.ds(mine * half, half), :] = inputs[at][:half, :]
            packed[pl.ds((1 - mine) * half, half), :] = inputs[at + 1][:half, :]
            listed = inputs[at][half : half + 1, :width].astype(jnp.int32)
            one_hot_into(members, column, listed)
            at += 2
        stacked = jnp.concatenate(
            [part for x in (packed[:, :width], packed[:, width:]) for part in split3(x)] + [ones],
            axis=0,
        )
        wide = dot_t(stacked, members[...])
        rows = slice(place * pixels, (place + 1) * pixels)
        first[rows, :] = join3(wide[: 3 * pixels])
        right[rows, :] = join3(wide[3 * pixels : 6 * pixels])
        keep[8 * place : 8 * place + 8, :] = wide[6 * pixels : 6 * pixels + 8]


def sweep_kernel(sizes, perm, weights, *refs):
    parts = len(sizes)
    firsts, rights, keeps = refs[:parts], refs[parts : 2 * parts], refs[2 * parts : 3 * parts]
    out_ref, cur, ahead, fresh, result = refs[3 * parts :]
    neurons = perm.shape[0]
    pixels = result.shape[0]
    blocks = neurons // BLK
    n = sum(sizes)
    where = [(part, place) for part, size in enumerate(sizes) for place in range(size)]
    total = n * pixels

    def tile(block):
        return slice(2 * block * BLK, 2 * (block + 1) * BLK)

    def look_ahead(block, spans, slot):
        for start in range(0, total, CHUNK):
            rows = slice(start, start + CHUNK)
            terms = [
                dot(cur[rows, 2 * lower * BLK : 2 * upper * BLK],
                    weights[2 * lower * BLK : 2 * upper * BLK, tile(block)])
                for lower, upper in spans if upper > lower
            ]
            if terms:
                both = sum(terms[1:], terms[0])
                ahead[slot, rows, :] = both[:, :BLK] + both[:, BLK:]

    def step(block, previous, has_ahead, source, next_block, next_spans):
        lower, upper = block * BLK, (block + 1) * BLK
        squares = jnp.zeros((8, BLK), f32)
        if previous is not None:
            for start in range(0, total, CHUNK):
                rows = slice(start, start + CHUNK)
                both = dot(cur[rows, tile(previous)], weights[tile(previous), tile(block)])
                fresh[rows, :] = both[:, :BLK] + both[:, BLK:]
        for s in range(n):
            rows = slice(s * pixels, (s + 1) * pixels)
            part, place = where[s]
            value = source[part][place * pixels : (place + 1) * pixels, lower:upper]
            if has_ahead:
                value = value - ahead[block % 2, rows, :]
            if previous is not None:
                value = value - fresh[rows, :]
            kept = keeps[part][8 * place : 8 * place + 1, lower:upper]
            value = kept * jnp.maximum(value, 0.0)
            fresh[rows, :] = value
            squares += jnp.sum((value * value).reshape(pixels // 8, 8, BLK), axis=0)
        if next_block is not None:
            look_ahead(next_block, next_spans, next_block % 2)
        mean = jnp.sum(squares, axis=0, keepdims=True) / total
        inverse = 1.0 / jnp.sqrt(mean + 1e-06)
        for s in range(n):
            rows = slice(s * pixels, (s + 1) * pixels)
            value = fresh[rows, :] * inverse
            if s == 0:
                result[:, lower:upper] = value
            hi, lo = split2(value)
            cur[rows, 2 * lower : 2 * lower + BLK] = hi
            cur[rows, 2 * lower + BLK : 2 * upper] = lo

    last = blocks - 1
    for block in range(blocks):
        previous = block - 1 if block else None
        if block < last:
            step(block, previous, block > 1, firsts, block + 1, [(0, block)])
        else:
            step(block, previous, block > 1, firsts, 0, [(0, last)])

    @pl.loop(0, SWEEPS - 1)
    def _(_):
        for block in range(blocks):
            after = (block + 1) % blocks
            spans = [(0, block), (block + 1, blocks)]
            step(block, (block - 1) % blocks, True, rights, after, spans)

    out_ref[...] = join3(dot(jnp.concatenate(split3(result[...]), axis=0), perm[...]))


def replicated(n, m, frames_y, traces, footprints, order, support):
    pixels, frames = frames_y.shape
    rows = traces.shape[0]
    neurons = footprints.shape[1]
    width = support.shape[1]

    def swap(x, dp, df):
        pairs = [(p * m + f, (p ^ dp) * m + (f ^ df)) for p in range(n) for f in range(m)]
        return lax.ppermute(x, ("pix", "frm"), pairs)

    def stack(xs):
        return jnp.concatenate(xs, axis=0) if len(xs) > 1 else xs[0]

    shape = jax.ShapeDtypeStruct
    vmem = pl.BlockSpec(memory_space=pltpu.VMEM)
    total = n * pixels

    def call(kernel, flops, outs, scratch, limit, *args):
        moving = sum(x.size * x.dtype.itemsize for x in args)
        return pl.pallas_call(
            kernel,
            out_shape=outs,
            in_specs=[vmem] * len(args),
            out_specs=jax.tree.map(lambda _: vmem, outs),
            scratch_shapes=[pltpu.VMEM(*x) for x in scratch],
            compiler_params=pltpu.CompilerParams(vmem_limit_bytes=limit * VMEM_BYTES // 60),
            cost_estimate=pl.CostEstimate(flops=flops, bytes_accessed=moving, transcendentals=0),
        )(*args)

    order_row = order.reshape(1, neurons)
    natural = lax.iota(jnp.int32, neurons).reshape(1, neurons)
    bits = [1 << k for k in range(n.bit_length() - 2, 0, -1)]
    far = {0: traces}
    for bit in bits:
        far[bit] = swap(traces, bit, 0)
    blobs, y = [], {0: frames_y}

    def beside(names, blob):
        blobs.append(([(s, g ^ 1) for s, g in names], swap(blob, 0, 1)))

    def named(group, ds, dg):
        return [(s ^ ds, dg) for s in group]

    def spread_near(group, blob, way):
        along = swap(blob, 1, 0)
        near, relays = [(named(group, 1, 0), along)], []
        for g in range(2, m, 2):
            across = swap(blob, 0, g)
            near.append((named(group, 0, g), across))
            if way == "direct":
                near.append((named(group, 1, g), swap(blob, 1, g)))
            else:
                hop = (across, 1, 0) if way == "x" else (along, 0, g)
                relays.append((named(group, 1, g), hop))
        return near, relays

    own_near, own_relays = spread_near([0], traces, "y")
    for g in range(2, m, 2):
        y[g] = swap(frames_y, 0, g)
    singles = []
    for bit in bits[1:]:
        for s in [s for s in far if s & -s > bit]:
            far[s ^ bit] = swap(far[s], bit, 0)
            singles.append(s ^ bit)
    pair, relays = [], []
    if bits:
        pair_blob = stack([far[bit] for bit in bits])
        pair, relays = spread_near(bits, pair_blob, "x")
    own_near += [(names, swap(*hop)) for names, hop in own_relays]
    beside([(0, 0)], traces)
    for g in range(0, m, 2):
        y[g + 1] = swap(y[g], 0, 1)
    if bits:
        beside(named(bits, 0, 0), pair_blob)
        blobs.append((named(bits, 0, 0), pair_blob))
    later = []
    for s in singles:
        near, _ = spread_near([s], far[s], "direct")
        later += near
        beside([(s, 0)], far[s])
        blobs.append(([(s, 0)], far[s]))
    pair += [(names, swap(*hop)) for names, hop in relays]
    column, perm, members, foot_hl, listed, own_frames, traces_here = call(
        setup_kernel,
        6 * pixels * neurons * neurons,
        (
            shape((neurons, LANES), jnp.int32),
            shape((neurons, neurons), bf16),
            shape((neurons, width), bf16),
            shape((2 * pixels, neurons), bf16),
            shape((EXTRA, 2 * width), f32),
            shape((pixels, frames), bf16),
            shape((rows, frames), bf16),
        ),
        [],
        16,
        order_row, natural, support, footprints, frames_y, traces,
    )
    for entry in own_near + pair + later:
        beside(*entry)
    blobs += [([(0, 0)], traces_here)] + own_near + pair + later

    g, own, mine = call(
        functools.partial(gram_kernel, m, [names for names, _ in blobs], rows),
        4 * neurons * neurons * m * frames,
        (
            shape((neurons, 2 * neurons), bf16),
            shape((pixels, 2 * width), f32),
            shape((pixels // 2 + EXTRA, 2 * width), f32),
        ),
        [
            ((m, neurons, frames), bf16),
            ((m, pixels, frames), bf16),
            ((neurons, m * frames), bf16),
            ((neurons, neurons), f32),
            ((6 * pixels, neurons), bf16),
        ],
        36,
        perm, members, foot_hl, listed,
        own_frames,
        *[y[k] for k in range(1, m)],
        *[blob for _, blob in blobs],
    )

    def unpack(group):
        args, halves = [column], []
        for s in group:
            args += [got[s], others[s]] if s else [own, members, g]
            halves.append(s == 0)
        size = len(group) * pixels
        outs = (
            shape((size, neurons), f32),
            shape((size, neurons), f32),
            shape((8 * len(group), neurons), f32),
        )
        if 0 in group:
            outs += (shape((2 * neurons, 2 * neurons), bf16),)
        flops = 14 * size * width * neurons
        scratch = [((neurons, width), bf16), ((pixels, 2 * width), f32)]
        kernel = functools.partial(unpack_kernel, halves, len(args) - 1)
        return call(kernel, flops, outs, scratch, UNPACK_MIB, *args)

    got, others, groups = {0: mine}, {}, []
    for bit in bits:
        got[bit] = swap(mine, bit, 0)
    got[1] = swap(mine, 1, 0)
    for bit in bits[::-1]:
        got[bit ^ 1] = swap(got[bit], 1, 0)
        if bit != bits[0]:
            for s in [s for s in list(got) if s & -s > bit]:
                got[s ^ bit] = swap(got[s], bit, 0)
    early = [1, bits[-1]] if bits else [1]
    for s in early:
        others[s] = swap(got[s], 0, 1)
    missing = [s ^ 1 for s in got if s ^ 1 not in got]
    for s in missing:
        got[s] = swap(got[s ^ 1], 1, 0)
    rest = [s for s in got if s and s not in others]
    for s in rest:
        others[s] = swap(got[s], 0, 1)
    groups = [[0], early, [s for s in got if s and s not in early]]
    groups = [group for group in groups if group]
    parts = [unpack(group) for group in groups]
    return call(
        functools.partial(sweep_kernel, [len(group) for group in groups]),
        2 * SWEEPS * 4 * total * neurons * neurons,
        shape((pixels, neurons), f32),
        [
            ((total, 2 * neurons), bf16),
            ((2, total, BLK), f32),
            ((total, BLK), f32),
            ((pixels, neurons), f32),
        ],
        SWEEP_MIB,
        perm, parts[0][3],
        *[part[0] for part in parts],
        *[part[1] for part in parts],
        *[part[2] for part in parts],
    )


def power_of_two(x):
    return x > 1 and x & (x - 1) == 0


def solution(mesh):
    n, m = mesh.shape["pix"], mesh.shape["frm"]

    def local(frames_y, traces, footprints, order, support):
        neurons = footprints.shape[1]
        total = n * frames_y.shape[0]
        fits = 12 * total * neurons + 10 * neurons * neurons <= VMEM_BYTES // 2
        lined = neurons % 256 == 0 and traces.shape[0] % LANES == 0
        if fits and lined and power_of_two(n) and power_of_two(m):
            return replicated(n, m, frames_y, traces, footprints, order, support)
        return spread(frames_y, traces, footprints, order, support)

    in_specs = (P("pix", "frm"), P("pix", "frm"), P("pix", None), P(), P("pix", None))
    out_specs = P("pix", None)
    return jax.shard_map(local, mesh=mesh, in_specs=in_specs, out_specs=out_specs, check_vma=False)
```
